256 devices in a mesh: dp: 8 (over z), expert: 32 (over x, y, core).
Axes of the slice: x: 4, y: 4, z: 8, core: 2. Of those that a mesh axis runs over, the one named last changes fastest.
Arguments:
- tokens: bfloat16 [16384, 2048], P(('dp', 'expert')), may hold values from -6 to 6
- norm_gain: bfloat16 [2048], replicated, may hold values from 0.099609375 to 1.8984375
- router_weight: bfloat16 [2048, 32], replicated, may hold values from -0.125 to 0.125
- gate_weight: bfloat16 [32, 2048, 5120], P('expert', None, 'dp'), may hold values from -0.125 to 0.125
- up_weight: bfloat16 [32, 2048, 5120], P('expert', None, 'dp'), may hold values from -0.125 to 0.125
- down_weight: bfloat16 [32, 5120, 2048], P('expert', 'dp'), may hold values from -0.078125 to 0.078125
- expert_picks: int32 [8, 32, 128], P('dp'), may hold values from 0 to 2047, as said below
- final_gain: bfloat16 [2048], replicated, may hold values from 0.099609375 to 1.8984375
- kv_weight: bfloat16 [2048, 32, 6, 2, 64], P(None, 'expert'), may hold values from -0.125 to 0.125
Outputs:
- moe_out: bfloat16 [16384, 2048], P(('dp', 'expert'))
- kv_cache: bfloat16 [16384, 32, 6, 2, 64], P('dp', 'expert')
The draws below stay inside these ranges and needn't reach their ends.
Inputs may be any that keep to these rules, and one draw needn't show every extreme that they name: `expert_picks`: for each group and expert, 128 different positions in the group. Of the 64 tokens of one device (positions s * 64 to (s + 1) * 64 - 1) one expert picks at most 8, and for every group and expert some device's tokens are picked exactly 8 times.
All inputs are finite; a program needn't handle non-finite values.
Results may differ from the reference program's by a relative error of at most 0.013.
Values may be sent and summed in bfloat16 or wider, within the bound.
A program may use at most 128 MiB of HBM per device.

```python
import jax
import jax.numpy as jnp
from jax import lax

D = 2048
FF = 5120
DK = 64
TOK_DEV = 64
LAYERS = 6
EXPERTS = 32
HEADS = 32
TOKENS = 16384
CAP = 128
MOST = 8
N_DP = 8
N_EXPERT = 32


def one_expert_picks(sub_key):
    key_full, key_slot, key_perm, key_order = jax.random.split(sub_key, 4)
    full_shard = jax.random.randint(key_full, (), 0, N_EXPERT)
    scores = jax.random.permutation(key_slot, N_EXPERT * MOST).astype(jnp.int32)
    shard_of = jnp.arange(N_EXPERT * MOST, dtype=jnp.int32) // MOST
    scores = jnp.where(shard_of == full_shard, scores - N_EXPERT * MOST, scores)
    chosen = jnp.argsort(scores, stable=True)[:CAP].astype(jnp.int32)
    shard_pos = chosen // MOST
    within = chosen % MOST
    shard_perms = jax.vmap(lambda perm_key: jax.random.permutation(perm_key, TOK_DEV))(jax.random.split(key_perm, N_EXPERT))
    token_pos = shard_pos * TOK_DEV + shard_perms[shard_pos, within].astype(jnp.int32)
    pick_order = jax.random.permutation(key_order, CAP)
    return token_pos[pick_order].astype(jnp.int32)


def draw_expert_picks(key, part):
    base = jax.random.fold_in(key, 7)
    keys = jax.random.split(base, N_DP * EXPERTS)
    all_picks = jax.vmap(one_expert_picks)(keys)
    return all_picks.reshape(N_DP, EXPERTS, CAP).astype(jnp.int32)


def levels(own_key, shape, shards, smallest, high):
    def one(axis_at, parts):
        draws = jax.random.uniform(jax.random.fold_in(jax.random.fold_in(own_key, 6), axis_at), (parts,), jnp.float32, smallest / len(shards), high / len(shards))
        return jnp.repeat(jnp.exp(draws), shape[axis_at] // parts).reshape((-1,) + (1,) * (len(shape) - axis_at - 1))

    level = one(*shards[0])
    for cut in shards[1:]:
        level = level * one(*cut)
    return level


def gaussian(key, dims, scale, bound, cuts=(), kind=jnp.bfloat16):
    level = levels(key, dims, cuts, -0.22, 0.18) if cuts else 1.0
    entries = jax.random.normal(key, dims, jnp.float32) * scale * level
    return jnp.minimum(jnp.maximum(entries, -bound), bound).astype(kind)


def setup_inputs(seed: int = 0) -> dict:
    key_list = jax.random.split(jax.random.key(seed), 10)
    tokens = gaussian(key_list[0], (TOKENS, D), 1.0, 6.0, ((0, 256),))
    norm_gain = jnp.clip(1.0 + 0.18 * jax.random.normal(key_list[1], (D,), jnp.float32), 0.099609375, 1.8984375).astype(jnp.bfloat16)
    router_weight = gaussian(key_list[2], (D, EXPERTS), D ** -0.5, 0.125)
    gate_weight = gaussian(key_list[3], (EXPERTS, D, FF), D ** -0.5, 0.125, ((0, 32), (2, 8)))
    up_weight = gaussian(key_list[4], (EXPERTS, D, FF), D ** -0.5, 0.125, ((0, 32), (2, 8)))
    down_weight = gaussian(key_list[5], (EXPERTS, FF, D), FF ** -0.5, 0.078125, ((0, 32), (1, 8)))
    expert_picks = draw_expert_picks(jax.random.fold_in(key_list[9], 71), 0)
    final_gain = jnp.clip(1.0 + 0.18 * jax.random.normal(key_list[7], (D,), jnp.float32), 0.099609375, 1.8984375).astype(jnp.bfloat16)
    kv_weight = gaussian(key_list[8], (D, HEADS, LAYERS, 2, DK), D ** -0.5, 0.125, ((1, 32),))
    return {"tokens": tokens, "norm_gain": norm_gain, "router_weight": router_weight, "gate_weight": gate_weight, "up_weight": up_weight, "down_weight": down_weight, "expert_picks": expert_picks, "final_gain": final_gain, "kv_weight": kv_weight}


def normalize(values, gain):
    return values * lax.rsqrt(lax.optimization_barrier(jnp.mean(values * values, axis=-1, keepdims=True)) + 1e-06) * gain.astype(jnp.float32)

def reference(tokens, norm_gain, router_weight, gate_weight, up_weight, down_weight, expert_picks, final_gain, kv_weight):
    wide_tokens = tokens.astype(jnp.float32)
    normed = normalize(wide_tokens, norm_gain).astype(jnp.bfloat16)
    gate_probs = jax.nn.sigmoid(jnp.dot(normed, router_weight, preferred_element_type=jnp.float32))
    group_start = jnp.arange(N_DP, dtype=jnp.int32)[:, None, None] * (TOK_DEV * N_EXPERT)
    all_rows = jnp.transpose(group_start + expert_picks, (1, 0, 2)).reshape(EXPERTS, -1).astype(jnp.int32)
    block_width = FF // N_DP

    def one_expert(expert):
        row_index = lax.dynamic_index_in_dim(all_rows, expert, 0, keepdims=False)
        inputs = normed[row_index]
        gate_act = jnp.dot(inputs, gate_weight[expert], preferred_element_type=jnp.float32)
        up_act = jnp.dot(inputs, up_weight[expert], preferred_element_type=jnp.float32)
        hidden = (jax.nn.gelu(gate_act, approximate=True) * up_act).astype(jnp.bfloat16)
        down_here = down_weight[expert]
        total = jnp.zeros((hidden.shape[0], D), jnp.float32)
        for block in range(N_DP):
            partial_sum = jnp.dot(hidden[:, block * block_width:(block + 1) * block_width], down_here[block * block_width:(block + 1) * block_width], preferred_element_type=jnp.float32).astype(jnp.bfloat16)
            partial_sum = lax.optimization_barrier(partial_sum)
            total = total + partial_sum.astype(jnp.float32)
        result = total.astype(jnp.bfloat16)
        weight = gate_probs[row_index, expert]
        return result.astype(jnp.float32) * weight[:, None]
    contributions = lax.map(one_expert, jnp.arange(EXPERTS, dtype=jnp.int32))
    combined = jnp.zeros((TOKENS, D), jnp.float32).at[all_rows.reshape(-1)].add(contributions.reshape(-1, D))
    moe_out = (wide_tokens + combined).astype(jnp.bfloat16)
    encoded = normalize(moe_out.astype(jnp.float32), final_gain).astype(jnp.bfloat16)
    projected = jnp.dot(encoded, kv_weight.reshape(D, -1), preferred_element_type=jnp.float32).astype(jnp.bfloat16)
    kv_cache = projected.reshape(TOKENS, HEADS, LAYERS, 2, DK)
    return (moe_out, kv_cache)
```

```python
import jax
import jax.numpy as jnp
from jax import lax
from jax.experimental import pallas as pl
from jax.experimental.pallas import tpu as pltpu
from jax.sharding import PartitionSpec as P

MESH = pl.DeviceIdType.MESH
PLACE = {0: 0, 1: 1, 7: 2, 2: 3, 6: 4, 3: 5, 5: 6, 4: 7}
RS_RIGHT = ((3, 1), (4, 0), (2, 1), (3, 0), (1, 1), (2, 0), (1, 0))
RS_LEFT = tuple(((8 - r) % 8, 1 - h) for r, h in RS_RIGHT)


def ring_kernel(picked, gate_w, up_w, down_w, out, wgu, wdn, rows, hid, part, landed,
                w_sem, own_sem, ag_send, ag_recv, rs_send, rs_recv):
    me = lax.axis_index("dp")
    n = lax.axis_size("dp")
    right = lax.rem(me + 1, n)
    left = lax.rem(me + n - 1, n)
    half = picked.shape[0] // 2
    blk = 2 * half
    tiles = wgu.shape[0]
    lanes = wgu.shape[2] // 2

    loads = []
    for j in range(tiles):
        cols = pl.ds(j * lanes, lanes)
        loads.append(pltpu.make_async_copy(gate_w.at[0, :, cols], wgu.at[j, :, pl.ds(0, lanes)], w_sem.at[2 * j]))
        loads.append(pltpu.make_async_copy(up_w.at[0, :, cols], wgu.at[j, :, pl.ds(lanes, lanes)], w_sem.at[2 * j + 1]))
    loads.append(pltpu.make_async_copy(down_w.at[0], wdn, w_sem.at[2 * tiles]))
    own = pltpu.make_async_copy(picked, rows.at[pl.ds(0, blk)], own_sem)
    own.start()
    for c in loads:
        c.start()

    barrier = pltpu.get_barrier_semaphore()
    for nb in (left, right):
        pl.semaphore_signal(barrier, inc=1, device_id={"dp": nb}, device_id_type=MESH)
    pl.semaphore_wait(barrier, 2)
    own.wait()

    def rows_at(r, h):
        return pl.ds(PLACE[r] * blk + h * half, half)

    def ag_copy(d, i):
        k = i // 2
        if d == 0:
            h = i % 2
            src, dst = (8 - k) % 8, (7 - k) % 8
        else:
            h = 1 - i % 2
            src, dst = k, k + 1
        return pltpu.make_async_remote_copy(
            src_ref=rows.at[rows_at(src, h)], dst_ref=rows.at[rows_at(dst, h)],
            send_sem=ag_send.at[d, i], recv_sem=ag_recv.at[d, i],
            device_id={"dp": (right, left)[d]}, device_id_type=MESH)

    ag = [[ag_copy(d, i) for i in range(7)] for d in range(2)]

    def rs_copy(d, i):
        r, h = (RS_RIGHT, RS_LEFT)[d][i]
        return pltpu.make_async_remote_copy(
            src_ref=part.at[rows_at(r, h)], dst_ref=landed.at[d, i],
            send_sem=rs_send.at[d, i], recv_sem=rs_recv.at[d, i],
            device_id={"dp": (right, left)[d]}, device_id_type=MESH)

    rs = [[rs_copy(d, i) for i in range(7)] for d in range(2)]

    def ffn(start, m):
        x = rows[pl.ds(start, m), :]
        for j in range(tiles):
            acc = jnp.dot(x, wgu[j], preferred_element_type=jnp.float32)
            hid[pl.ds(0, m), pl.ds(j * lanes, lanes)] = (
                jax.nn.gelu(acc[:, :lanes], approximate=True) * acc[:, lanes:]
            ).astype(jnp.bfloat16)
        width = wdn.shape[1] // 4
        for j in range(4):
            cols = pl.ds(j * width, width)
            part[pl.ds(start, m), cols] = jnp.dot(
                hid[pl.ds(0, m), :], wdn[:, cols], preferred_element_type=jnp.float32
            ).astype(jnp.bfloat16)

    for i in range(2):
        for d in range(2):
            ag[d][i].start()
    for c in loads:
        c.wait()
    ffn(0, blk)
    for k in range(1, 4):
        for i in (2 * k - 2, 2 * k - 1):
            for d in range(2):
                ag[d][i].wait_recv()
                if i + 2 < 7:
                    ag[d][i + 2].start()
        ffn(blk + 2 * blk * (k - 1), 2 * blk)
    for d in range(2):
        rs[d][0].start()
    for d in range(2):
        ag[d][6].wait_recv()
    ffn(7 * blk, blk)
    for d in range(2):
        rs[d][1].start()
    for i in range(7):
        for d in range(2):
            rs[d][i].wait_recv()
            order = (RS_RIGHT, RS_LEFT)[d]
            r, h = order[i]
            r = (r - 1 + 2 * d) % 8
            if r == 0:
                continue
            at = rows_at(r, h)
            part[at, :] = (part[at, :].astype(jnp.float32) + landed[d, i].astype(jnp.float32)).astype(jnp.bfloat16)
            rs[d][order.index((r, h))].start()
    for h in range(2):
        at = pl.ds(h * half, half)
        total = part[at, :].astype(jnp.float32)
        for d in range(2):
            i = 6 if d == h else 4
            total = total + landed[d, i].astype(jnp.float32)
        out[at, :] = total.astype(jnp.bfloat16)
    for d in range(2):
        for i in range(7):
            ag[d][i].wait_send()
            rs[d][i].wait_send()


def expert_ffn(picked, gate_weight, up_weight, down_weight):
    blk, dim = picked.shape
    ff = gate_weight.shape[2]
    lanes = 128
    tiles = ff // lanes
    return pl.pallas_call(
        ring_kernel,
        out_shape=jax.ShapeDtypeStruct((blk, dim), jnp.bfloat16),
        in_specs=[pl.BlockSpec(memory_space=pl.ANY)] * 4,
        out_specs=pl.BlockSpec(memory_space=pltpu.VMEM),
        scratch_shapes=[
            pltpu.VMEM((tiles, dim, 2 * lanes), jnp.bfloat16),
            pltpu.VMEM((ff, dim), jnp.bfloat16),
            pltpu.VMEM((8 * blk, dim), jnp.bfloat16),
            pltpu.VMEM((2 * blk, ff), jnp.bfloat16),
            pltpu.VMEM((8 * blk, dim), jnp.bfloat16),
            pltpu.VMEM((2, 7, blk // 2, dim), jnp.bfloat16),
            pltpu.SemaphoreType.DMA((2 * tiles + 1,)),
            pltpu.SemaphoreType.DMA,
            pltpu.SemaphoreType.DMA((2, 7)),
            pltpu.SemaphoreType.DMA((2, 7)),
            pltpu.SemaphoreType.DMA((2, 7)),
            pltpu.SemaphoreType.DMA((2, 7)),
        ],
        compiler_params=pltpu.CompilerParams(
            collective_id=0, has_side_effects=True, vmem_limit_bytes=60 * 1024 * 1024
        ),
        name="ring_ffn",
    )(picked, gate_weight, up_weight, down_weight)


def normalize(values, gain):
    return (
        values
        * lax.rsqrt(jnp.mean(values * values, axis=-1, keepdims=True) + 1e-06)
        * gain.astype(jnp.float32)
    )


def local(
    tokens,
    norm_gain,
    router_weight,
    gate_weight,
    up_weight,
    down_weight,
    expert_picks,
    final_gain,
    kv_weight,
):
    expert_count = lax.axis_size("expert")
    own_index = lax.axis_index("expert")
    tok_rows = tokens.shape[0]
    wide_tokens = tokens.astype(jnp.float32)
    normed = normalize(wide_tokens, norm_gain).astype(jnp.bfloat16)
    gate_probs = jax.nn.sigmoid(jnp.dot(normed, router_weight, preferred_element_type=jnp.float32))
    chosen = expert_picks[0]
    capacity = chosen.shape[1]
    slot_count = 4 * tok_rows // expert_count
    source = chosen // tok_rows
    local_row = chosen % tok_rows
    positions = jnp.arange(capacity, dtype=jnp.int32)
    earlier = (source[:, :, None] == source[:, None, :]) & (
        positions[None, None, :] < positions[None, :, None]
    )
    slot_rank = jnp.sum(earlier.astype(jnp.int32), axis=2)
    slot_ids = jnp.arange(slot_count, dtype=jnp.int32)
    shard_ids = jnp.arange(expert_count, dtype=jnp.int32)
    own_source = lax.dynamic_index_in_dim(source, own_index, 0, keepdims=False)
    own_rank = lax.dynamic_index_in_dim(slot_rank, own_index, 0, keepdims=False)
    compact_map = (
        (own_source[:, None, None] == shard_ids[None, :, None])
        & (own_rank[:, None, None] == slot_ids[None, None, :])
    ).astype(jnp.bfloat16)
    send_slot = (
        (source == own_index)[:, :, None] & (slot_rank[:, :, None] == slot_ids[None, None, :])
    ).astype(jnp.bfloat16)
    local_map = (
        local_row[:, :, None] == jnp.arange(tok_rows, dtype=jnp.int32)[None, None, :]
    ).astype(jnp.bfloat16)
    send_map = jnp.einsum("ecm,ect->emt", send_slot, local_map, preferred_element_type=jnp.float32)
    outgoing = jnp.einsum(
        "emt,td->emd", send_map.astype(jnp.bfloat16), normed, preferred_element_type=jnp.float32
    ).astype(jnp.bfloat16)
    incoming = lax.all_to_all(outgoing, "expert", split_axis=0, concat_axis=0, tiled=True)
    picked = jnp.einsum(
        "csm,smd->cd", compact_map, incoming, preferred_element_type=jnp.float32
    ).astype(jnp.bfloat16)
    summed = expert_ffn(picked, gate_weight, up_weight, down_weight)
    outbound = jnp.einsum(
        "csm,cd->smd", compact_map, summed, preferred_element_type=jnp.float32
    ).astype(jnp.bfloat16)
    returned = lax.all_to_all(outbound, "expert", split_axis=0, concat_axis=0, tiled=True)
    combine_weight = jnp.transpose(send_map, (2, 0, 1)) * gate_probs[:, :, None]
    combined = jnp.einsum("tem,emd->td", combine_weight, returned.astype(jnp.float32))
    moe_out = (wide_tokens + combined).astype(jnp.bfloat16)
    encoded = normalize(moe_out.astype(jnp.float32), final_gain).astype(jnp.bfloat16)
    kv_matrix = kv_weight.reshape(kv_weight.shape[0], -1)
    kv_rows = jnp.dot(
        lax.all_gather(encoded, "expert", axis=0, tiled=True),
        kv_matrix,
        preferred_element_type=jnp.float32,
    ).astype(jnp.bfloat16)
    kv_cache = kv_rows.reshape((kv_rows.shape[0],) + kv_weight.shape[1:])
    return (moe_out, kv_cache)


def solution(mesh):
    in_specs = (
        P(("dp", "expert"), None),
        P(),
        P(),
        P("expert", None, "dp"),
        P("expert", None, "dp"),
        P("expert", "dp", None),
        P("dp", None, None),
        P(),
        P(None, "expert", None, None, None),
    )
    out_specs = (P(("dp", "expert"), None), P("dp", "expert", None, None, None))
    return jax.shard_map(local, mesh=mesh, in_specs=in_specs, out_specs=out_specs, check_vma=False)
```

```python
import jax
import jax.numpy as jnp
from jax import lax
from jax.experimental import pallas as pl
from jax.experimental.pallas import tpu as pltpu
from jax.sharding import PartitionSpec as P

MESH = pl.DeviceIdType.MESH
PLACE = {0: 0, 1: 1, 7: 2, 2: 3, 6: 4, 3: 5, 5: 6, 4: 7}
RS_RIGHT = ((3, 1), (4, 0), (2, 1), (3, 0), (1, 1), (2, 0), (1, 0))
RS_LEFT = tuple(((8 - r) % 8, 1 - h) for r, h in RS_RIGHT)


def ring_kernel(picked, gate_w, up_w, down_w, out, wgu, wdn, rows, hid, part, landed,
                w_sem, own_sem, ag_send, ag_recv, rs_send, rs_recv):
    me = lax.axis_index("dp")
    n = lax.axis_size("dp")
    right = lax.rem(me + 1, n)
    left = lax.rem(me + n - 1, n)
    half = picked.shape[0] // 2
    blk = 2 * half
    tiles = wgu.shape[0]
    lanes = wgu.shape[2] // 2

    loads = []
    for j in range(tiles):
        cols = pl.ds(j * lanes, lanes)
        loads.append(pltpu.make_async_copy(gate_w.at[0, :, cols], wgu.at[j, :, pl.ds(0, lanes)], w_sem.at[2 * j]))
        loads.append(pltpu.make_async_copy(up_w.at[0, :, cols], wgu.at[j, :, pl.ds(lanes, lanes)], w_sem.at[2 * j + 1]))
    loads.append(pltpu.make_async_copy(down_w.at[0], wdn, w_sem.at[2 * tiles]))
    own = pltpu.make_async_copy(picked, rows.at[pl.ds(0, blk)], own_sem)
    own.start()
    for c in loads:
        c.start()

    barrier = pltpu.get_barrier_semaphore()
    for nb in (left, right):
        pl.semaphore_signal(barrier, inc=1, device_id={"dp": nb}, device_id_type=MESH)
    pl.semaphore_wait(barrier, 2)
    own.wait()

    def rows_at(r, h):
        return pl.ds(PLACE[r] * blk + h * half, half)

    def ag_copy(d, i):
        k = i // 2
        if d == 0:
            h = i % 2
            src, dst = (8 - k) % 8, (7 - k) % 8
        else:
            h = 1 - i % 2
            src, dst = k, k + 1
        return pltpu.make_async_remote_copy(
            src_ref=rows.at[rows_at(src, h)], dst_ref=rows.at[rows_at(dst, h)],
            send_sem=ag_send.at[d, i], recv_sem=ag_recv.at[d, i],
            device_id={"dp": (right, left)[d]}, device_id_type=MESH)

    ag = [[ag_copy(d, i) for i in range(7)] for d in range(2)]

    def rs_copy(d, i):
        r, h = (RS_RIGHT, RS_LEFT)[d][i]
        return pltpu.make_async_remote_copy(
            src_ref=part.at[rows_at(r, h)], dst_ref=landed.at[d, i],
            send_sem=rs_send.at[d, i], recv_sem=rs_recv.at[d, i],
            device_id={"dp": (right, left)[d]}, device_id_type=MESH)

    rs = [[rs_copy(d, i) for i in range(7)] for d in range(2)]

    def ffn(start, m):
        x = rows[pl.ds(start, m), :]
        for j in range(tiles):
            acc = jnp.dot(x, wgu[j], preferred_element_type=jnp.float32)
            hid[pl.ds(0, m), pl.ds(j * lanes, lanes)] = (
                jax.nn.gelu(acc[:, :lanes], approximate=True) * acc[:, lanes:]
            ).astype(jnp.bfloat16)
        width = wdn.shape[1] // 4
        for j in range(4):
            cols = pl.ds(j * width, width)
            part[pl.ds(start, m), cols] = jnp.dot(
                hid[pl.ds(0, m), :], wdn[:, cols], preferred_element_type=jnp.float32
            ).astype(jnp.bfloat16)

    for i in range(2):
        for d in range(2):
            ag[d][i].start()
    for c in loads:
        c.wait()
    ffn(0, blk)
    for k in range(1, 4):
        for i in (2 * k - 2, 2 * k - 1):
            for d in range(2):
                ag[d][i].wait_recv()
                if i + 2 < 7:
                    ag[d][i + 2].start()
        ffn(blk + 2 * blk * (k - 1), 2 * blk)
    for d in range(2):
        rs[d][0].start()
    for d in range(2):
        ag[d][6].wait_recv()
    ffn(7 * blk, blk)
    for d in range(2):
        rs[d][1].start()
    for i in range(7):
        for d in range(2):
            rs[d][i].wait_recv()
            order = (RS_RIGHT, RS_LEFT)[d]
            r, h = order[i]
            r = (r - 1 + 2 * d) % 8
            if r == 0:
                continue
            at = rows_at(r, h)
            part[at, :] = (part[at, :].astype(jnp.float32) + landed[d, i].astype(jnp.float32)).astype(jnp.bfloat16)
            rs[d][order.index((r, h))].start()
    for h in range(2):
        at = pl.ds(h * half, half)
        total = part[at, :].astype(jnp.float32)
        for d in range(2):
            i = 6 if d == h else 4
            total = total + landed[d, i].astype(jnp.float32)
        out[at, :] = total.astype(jnp.bfloat16)
    for d in range(2):
        for i in range(7):
            ag[d][i].wait_send()
            rs[d][i].wait_send()


def expert_ffn(picked, gate_weight, up_weight, down_weight):
    blk, dim = picked.shape
    ff = gate_weight.shape[2]
    lanes = 128
    tiles = ff // lanes
    return pl.pallas_call(
        ring_kernel,
        out_shape=jax.ShapeDtypeStruct((blk, dim), jnp.bfloat16),
        in_specs=[pl.BlockSpec(memory_space=pl.ANY)] * 4,
        out_specs=pl.BlockSpec(memory_space=pltpu.VMEM),
        scratch_shapes=[
            pltpu.VMEM((tiles, dim, 2 * lanes), jnp.bfloat16),
            pltpu.VMEM((ff, dim), jnp.bfloat16),
            pltpu.VMEM((8 * blk, dim), jnp.bfloat16),
            pltpu.VMEM((2 * blk, ff), jnp.bfloat16),
            pltpu.VMEM((8 * blk, dim), jnp.bfloat16),
            pltpu.VMEM((2, 7, blk // 2, dim), jnp.bfloat16),
            pltpu.SemaphoreType.DMA((2 * tiles + 1,)),
            pltpu.SemaphoreType.DMA,
            pltpu.SemaphoreType.DMA((2, 7)),
            pltpu.SemaphoreType.DMA((2, 7)),
            pltpu.SemaphoreType.DMA((2, 7)),
            pltpu.SemaphoreType.DMA((2, 7)),
        ],
        compiler_params=pltpu.CompilerParams(
            collective_id=0, has_side_effects=True, vmem_limit_bytes=60 * 1024 * 1024
        ),
        name="ring_ffn",
    )(picked, gate_weight, up_weight, down_weight)


SIDE = 4
ORDER = (0, 3, 1, 2)


def plane_kernel(encoded, kv_t, out, blocks, wkv, tile, in_sem, w_sem, out_sem,
                 send_sem, recv_sem, sub_send, sub_recv, twin_send, twin_recv):
    me = lax.axis_index("expert")
    core = lax.rem(me, 2)
    chip = lax.div(me, 2)
    pos = (lax.div(chip, SIDE), lax.rem(chip, SIDE))
    tok = encoded.shape[0]
    half = tok // 2
    sub = half // 2

    def shift(v, by):
        return lax.rem(v + by, SIDE)

    def member(x, y, c):
        return (x * SIDE + y) * 2 + c

    def coords(h, first, second):
        a, b = shift(pos[h], first), shift(pos[1 - h], second)
        return (a, b) if h == 0 else (b, a)

    def start_of(h, first, second, c):
        x, y = coords(h, first, second)
        return member(x, y, c) * tok + h * half

    load_w = pltpu.make_async_copy(kv_t, wkv, w_sem)
    own = pltpu.make_async_copy(encoded, blocks.at[pl.ds(me * tok, tok)], in_sem)
    own.start()
    load_w.start()
    peers = [member(*coords(h, f, 0), core) for h in range(2) for f in (1, 3)]
    twin = member(*pos, 1 - core)
    barrier = pltpu.get_barrier_semaphore()
    for p in peers + [twin]:
        pl.semaphore_signal(barrier, inc=1, device_id={"expert": p}, device_id_type=MESH)
    pl.semaphore_wait(barrier, 5)
    own.wait()

    started = []

    def remote(rows, n, send, recv, target):
        at = blocks.at[pl.ds(pl.multiple_of(rows, 16), n)]
        return pltpu.make_async_remote_copy(
            src_ref=at, dst_ref=at, send_sem=send, recv_sem=recv,
            device_id={"expert": target}, device_id_type=MESH)

    def go(c):
        c.start()
        started.append(c)

    def along_first(h, first, by):
        f = (first - by) % SIDE
        go(remote(start_of(h, first, 0, core), half, send_sem.at[h, f, 0, 0], recv_sem.at[h, f, 0],
                  member(*coords(h, by, 0), core)))

    def sub_along_first(h, first, by, part):
        go(remote(start_of(h, first, 0, core) + part * sub, sub, sub_send.at[h, part], sub_recv.at[h, part],
                  member(*coords(h, by, 0), core)))

    def along_second(h, first, second, by):
        s = (second - by) % SIDE
        go(remote(start_of(h, first, second, core), half, send_sem.at[h, first, s, 1], recv_sem.at[h, first, s],
                  member(*coords(h, 0, by), core)))

    def to_twin(h, first, second):
        go(remote(start_of(h, first, second, core), half, twin_send.at[h, first, second],
                  twin_recv.at[h, first, second], twin))

    def arrived(h, first, second):
        rows = start_of(h, first, second, core)
        if (first, second) == (2, 0):
            for part in range(2):
                remote(rows + part * sub, sub, sub_send.at[h, part], sub_recv.at[h, part], twin).wait_recv()
        else:
            remote(rows, half, send_sem.at[h, 0, 0, 0], recv_sem.at[h, first, second], twin).wait_recv()

    def twin_arrived(h, first, second):
        remote(start_of(h, first, second, 1 - core), half, twin_send.at[h, first, second],
               twin_recv.at[h, first, second], twin).wait_recv()

    def chip_ready(dx, dy):
        for h in range(2):
            twin_arrived(h, *((dx, dy) if h == 0 else (dy, dx)))

    stores = []

    def project(*chips):
        for dx, dy in chips:
            chip_ready(dx, dy)
        starts = [member(shift(pos[0], dx), shift(pos[1], dy), 0) * tok for dx, dy in chips]
        slot = len(stores) // 2
        x = jnp.concatenate([blocks[pl.ds(pl.multiple_of(s, 2 * tok), 2 * tok), :] for s in starts], axis=0)
        y = lax.dot_general(wkv[...], x, (((1,), (1,)), ((), ())), preferred_element_type=jnp.float32)
        tile[slot] = y.astype(jnp.bfloat16)
        for i, s in enumerate(starts):
            c = pltpu.make_async_copy(
                tile.at[slot, :, pl.ds(i * 2 * tok, 2 * tok)],
                out.at[:, pl.ds(pl.multiple_of(s, 2 * tok), 2 * tok)], out_sem.at[len(stores)])
            c.start()
            stores.append(c)

    for h in range(2):
        for by in (1, 3):
            along_first(h, 0, by)
    for h in range(2):
        for by in (1, 3):
            along_second(h, 0, 0, by)
    for h in range(2):
        to_twin(h, 0, 0)
    load_w.wait()
    for h in range(2):
        for f in (3, 1):
            arrived(h, f, 0)
            sub_along_first(h, f, (4 - f) % 4, 0 if f == 3 else 1)
            for by in (1, 3):
                along_second(h, f, 0, by)
            to_twin(h, f, 0)
    for s in (3, 1):
        for h in range(2):
            arrived(h, 0, s)
            if s == 3:
                along_second(h, 0, 3, 1)
            to_twin(h, 0, s)
    project((0, 0), (3, 0))
    for h in range(2):
        arrived(h, 2, 0)
        for by in (1, 3):
            along_second(h, 2, 0, by)
        to_twin(h, 2, 0)
    project((1, 0), (0, 3))
    for f in (3, 1):
        for s in (3, 1):
            for h in range(2):
                arrived(h, f, s)
                if (f, s) == (1, 3):
                    along_second(h, 1, 3, 1)
                if (f, s) == (3, 1):
                    along_second(h, 3, 1, 3)
                to_twin(h, f, s)
        if f == 3:
            project((0, 1), (3, 3))
    project((1, 1), (1, 3))
    for s in (3, 1):
        for h in range(2):
            arrived(h, 2, s)
            if s == 1:
                along_second(h, 2, 1, 3)
            to_twin(h, 2, s)
    for f, chips in ((0, ((3, 1), (2, 0))), (1, ((0, 2), (1, 2))), (3, ((2, 1), (3, 2))), (2, ((2, 3), (2, 2)))):
        for h in range(2):
            arrived(h, f, 2)
            to_twin(h, f, 2)
        project(*chips)
    for c in stores:
        c.wait()
    for c in started:
        c.wait_send()


def kv_projection(encoded, kv_t):
    tok, dim = encoded.shape
    width = kv_t.shape[0]
    count = 2 * SIDE * SIDE
    return pl.pallas_call(
        plane_kernel,
        out_shape=jax.ShapeDtypeStruct((width, count * tok), jnp.bfloat16),
        in_specs=[pl.BlockSpec(memory_space=pl.ANY)] * 2,
        out_specs=pl.BlockSpec(memory_space=pl.ANY),
        scratch_shapes=[
            pltpu.VMEM((count * tok, dim), jnp.bfloat16),
            pltpu.VMEM((width, dim), jnp.bfloat16),
            pltpu.VMEM((8, width, 4 * tok), jnp.bfloat16),
            pltpu.SemaphoreType.DMA,
            pltpu.SemaphoreType.DMA,
            pltpu.SemaphoreType.DMA((16,)),
            pltpu.SemaphoreType.DMA((2, 4, 4, 2)),
            pltpu.SemaphoreType.DMA((2, 4, 4)),
            pltpu.SemaphoreType.DMA((2, 2)),
            pltpu.SemaphoreType.DMA((2, 2)),
            pltpu.SemaphoreType.DMA((2, 4, 4)),
            pltpu.SemaphoreType.DMA((2, 4, 4)),
        ],
        compiler_params=pltpu.CompilerParams(
            collective_id=1, has_side_effects=True, vmem_limit_bytes=60 * 1024 * 1024
        ),
        name="plane_kv",
    )(encoded, kv_t)


def normalize(values, gain):
    return (
        values
        * lax.rsqrt(jnp.mean(values * values, axis=-1, keepdims=True) + 1e-06)
        * gain.astype(jnp.float32)
    )


def local(
    tokens,
    norm_gain,
    router_weight,
    gate_weight,
    up_weight,
    down_weight,
    expert_picks,
    final_gain,
    kv_weight,
):
    expert_count = lax.axis_size("expert")
    own_index = lax.axis_index("expert")
    tok_rows = tokens.shape[0]
    wide_tokens = tokens.astype(jnp.float32)
    normed = normalize(wide_tokens, norm_gain).astype(jnp.bfloat16)
    gate_probs = jax.nn.sigmoid(jnp.dot(normed, router_weight, preferred_element_type=jnp.float32))
    chosen = expert_picks[0]
    capacity = chosen.shape[1]
    slot_count = 4 * tok_rows // expert_count
    source = chosen // tok_rows
    local_row = chosen % tok_rows
    positions = jnp.arange(capacity, dtype=jnp.int32)
    earlier = (source[:, :, None] == source[:, None, :]) & (
        positions[None, None, :] < positions[None, :, None]
    )
    slot_rank = jnp.sum(earlier.astype(jnp.int32), axis=2)
    slot_ids = jnp.arange(slot_count, dtype=jnp.int32)
    shard_ids = jnp.arange(expert_count, dtype=jnp.int32)
    own_source = lax.dynamic_index_in_dim(source, own_index, 0, keepdims=False)
    own_rank = lax.dynamic_index_in_dim(slot_rank, own_index, 0, keepdims=False)
    compact_map = (
        (own_source[:, None, None] == shard_ids[None, :, None])
        & (own_rank[:, None, None] == slot_ids[None, None, :])
    ).astype(jnp.bfloat16)
    send_slot = (
        (source == own_index)[:, :, None] & (slot_rank[:, :, None] == slot_ids[None, None, :])
    ).astype(jnp.bfloat16)
    local_map = (
        local_row[:, :, None] == jnp.arange(tok_rows, dtype=jnp.int32)[None, None, :]
    ).astype(jnp.bfloat16)
    send_map = jnp.einsum("ecm,ect->emt", send_slot, local_map, preferred_element_type=jnp.float32)
    outgoing = jnp.einsum(
        "emt,td->emd", send_map.astype(jnp.bfloat16), normed, preferred_element_type=jnp.float32
    ).astype(jnp.bfloat16)
    incoming = lax.all_to_all(outgoing, "expert", split_axis=0, concat_axis=0, tiled=True)
    picked = jnp.einsum(
        "csm,smd->cd", compact_map, incoming, preferred_element_type=jnp.float32
    ).astype(jnp.bfloat16)
    summed = expert_ffn(picked, gate_weight, up_weight, down_weight)
    outbound = jnp.einsum(
        "csm,cd->smd", compact_map, summed, preferred_element_type=jnp.float32
    ).astype(jnp.bfloat16)
    returned = lax.all_to_all(outbound, "expert", split_axis=0, concat_axis=0, tiled=True)
    combine_weight = jnp.transpose(send_map, (2, 0, 1)) * gate_probs[:, :, None]
    combined = jnp.einsum("tem,emd->td", combine_weight, returned.astype(jnp.float32))
    moe_out = (wide_tokens + combined).astype(jnp.bfloat16)
    encoded = normalize(moe_out.astype(jnp.float32), final_gain).astype(jnp.bfloat16)
    heads = kv_weight.shape[1:]
    kv_t = kv_weight.transpose(1, 2, 3, 4, 0).reshape(-1, kv_weight.shape[0])
    kv_rows = kv_projection(encoded, kv_t)
    kv_cache = kv_rows.reshape(heads + (kv_rows.shape[1],)).transpose(4, 0, 1, 2, 3)
    return (moe_out, kv_cache)


def solution(mesh):
    in_specs = (
        P(("dp", "expert"), None),
        P(),
        P(),
        P("expert", None, "dp"),
        P("expert", None, "dp"),
        P("expert", "dp", None),
        P("dp", None, None),
        P(),
        P(None, "expert", None, None, None),
    )
    out_specs = (P(("dp", "expert"), None), P("dp", "expert", None, None, None))
    return jax.shard_map(local, mesh=mesh, in_specs=in_specs, out_specs=out_specs, check_vma=False)
```
